8 devices in a mesh: heads: 4 (over z, y, x), model: 2 (over core).
Axes of the slice: x: 2, y: 2, z: 1, core: 2. Of those that a mesh axis runs over, the one named last changes fastest.
Arguments:
- hidden_in: bfloat16 [6144, 2304], P(None, 'model')
- seg_ids: int32 [6144], replicated
- positions: int32 [6144], replicated
- w_query: bfloat16 [2, 2304, 2048], P(None, 'model', 'heads')
- w_key: bfloat16 [2, 2304, 1024], P(None, 'model', 'heads')
- w_value: bfloat16 [2, 2304, 1024], P(None, 'model', 'heads')
- w_out: bfloat16 [2, 2048, 2304], P(None, 'heads', 'model')
- w_gate: bfloat16 [2, 2304, 9216], P(None, 'model', 'heads')
- w_up: bfloat16 [2, 2304, 9216], P(None, 'model', 'heads')
- w_down: bfloat16 [2, 9216, 2304], P(None, 'heads', 'model')
- norm_scales: float32 [2, 4, 2304], P(None, None, 'model')
- qk_scales: float32 [2, 2, 256], replicated
Outputs:
- output 1: bfloat16 [6144, 2304], P(None, 'model')
- output 2: bfloat16 [2, 6144, 4, 256], P(None, None, 'heads')
- output 3: bfloat16 [2, 6144, 4, 256], P(None, None, 'heads')
All inputs are finite; a program needn't handle non-finite values.
Results may differ from the reference program's by a relative error of at most 0.02.
Values are sent between devices in bfloat16 or wider.
A program may use at most 1 GiB of HBM per device.

```python
import jax
import jax.numpy as jnp
from jax import lax

TOKENS = 6144
D_MODEL = 2304
Q_HEADS = 8
KV_HEADS = 4
HEAD_DIM = 256
FFN_DIM = 9216
WINDOW = 1024
REQUESTS = 8
Q_BLOCK = 256
OUTLIERS = 8
NORM_EPS = 1e-6
GLOBAL_BASE = 1000000.0
GLOBAL_FACTOR = 8.0
LOCAL_BASE = 10000.0


def draw_requests(rng_key):
    cut_points = jnp.sort(jax.random.permutation(rng_key, TOKENS - 1)[:REQUESTS - 1] + 1).astype(jnp.int32)
    tok_index = jnp.arange(TOKENS, dtype=jnp.int32)
    seg_ids = jnp.sum((tok_index[:, None] >= cut_points[None, :]).astype(jnp.int32), axis=1)
    starts = jnp.concatenate([jnp.zeros((1,), jnp.int32), cut_points])
    positions = tok_index - starts[seg_ids]
    return seg_ids.astype(jnp.int32), positions.astype(jnp.int32)


def gauss_weight(rng_key, arr_shape, fan_in):
    return jax.random.normal(rng_key, arr_shape, jnp.float32) * (fan_in ** -0.5)


def setup_inputs(seed: int = 0) -> dict:
    rng_keys = jax.random.split(jax.random.key(seed), 16)
    seg_ids, positions = draw_requests(rng_keys[0])
    col_scale = jnp.exp(0.6 * jax.random.normal(rng_keys[1], (D_MODEL,), jnp.float32))
    hot_cols = jax.random.permutation(rng_keys[2], D_MODEL)[:OUTLIERS]
    col_scale = col_scale.at[hot_cols].set(20.0)
    hidden = jax.random.normal(rng_keys[3], (TOKENS, D_MODEL), jnp.float32) * col_scale[None, :]
    hidden = hidden * lax.rsqrt(jnp.mean(hidden * hidden))
    q_width = Q_HEADS * HEAD_DIM
    kv_width = KV_HEADS * HEAD_DIM
    out_cols = jnp.exp(0.5 * jax.random.normal(rng_keys[4], (2, 1, D_MODEL), jnp.float32))
    down_cols = jnp.exp(0.5 * jax.random.normal(rng_keys[5], (2, 1, D_MODEL), jnp.float32))
    return {
        'hidden_in': hidden.astype(jnp.bfloat16),
        'seg_ids': seg_ids,
        'positions': positions,
        'w_query': gauss_weight(rng_keys[6], (2, D_MODEL, q_width), D_MODEL).astype(jnp.bfloat16),
        'w_key': gauss_weight(rng_keys[7], (2, D_MODEL, kv_width), D_MODEL).astype(jnp.bfloat16),
        'w_value': gauss_weight(rng_keys[8], (2, D_MODEL, kv_width), D_MODEL).astype(jnp.bfloat16),
        'w_out': (gauss_weight(rng_keys[9], (2, q_width, D_MODEL), q_width) * out_cols).astype(jnp.bfloat16),
        'w_gate': gauss_weight(rng_keys[10], (2, D_MODEL, FFN_DIM), D_MODEL).astype(jnp.bfloat16),
        'w_up': gauss_weight(rng_keys[11], (2, D_MODEL, FFN_DIM), D_MODEL).astype(jnp.bfloat16),
        'w_down': (gauss_weight(rng_keys[12], (2, FFN_DIM, D_MODEL), FFN_DIM) * down_cols).astype(jnp.bfloat16),
        'norm_scales': 0.5 * jax.random.normal(rng_keys[13], (2, 4, D_MODEL), jnp.float32),
        'qk_scales': 0.5 * jax.random.normal(rng_keys[14], (2, 2, HEAD_DIM), jnp.float32),
    }


def gemma_norm(values, scale_row):
    mean_sq = jnp.mean(values * values, axis=-1, keepdims=True)
    return values * lax.rsqrt(mean_sq + NORM_EPS) * (1.0 + scale_row)


def rope_tables(positions, rope_base, pos_factor):
    exponents = jnp.arange(0, HEAD_DIM, 2).astype(jnp.float32) / HEAD_DIM
    inv_freq = rope_base ** (-exponents)
    angles = (positions.astype(jnp.float32) / pos_factor)[:, None] * inv_freq[None, :]
    return jnp.cos(angles), jnp.sin(angles)


def apply_rope(values, cos_tab, sin_tab):
    half_dim = values.shape[-1] // 2
    first_half = values[..., :half_dim]
    second_half = values[..., half_dim:]
    cos_bcast = cos_tab[:, None, :]
    sin_bcast = sin_tab[:, None, :]
    return jnp.concatenate([first_half * cos_bcast - second_half * sin_bcast, second_half * cos_bcast + first_half * sin_bcast], axis=-1)


def attend(query_heads, key_heads, value_heads, seg_ids, positions, window):
    group_size = Q_HEADS // KV_HEADS
    n_blocks = TOKENS // Q_BLOCK
    q_scale = HEAD_DIM ** -0.5
    key_f32 = key_heads.astype(jnp.float32)
    value_f32 = value_heads.astype(jnp.float32)
    q_blocks = query_heads.reshape(n_blocks, Q_BLOCK, KV_HEADS, group_size, HEAD_DIM)
    seg_blocks = seg_ids.reshape(n_blocks, Q_BLOCK)
    pos_blocks = positions.reshape(n_blocks, Q_BLOCK)

    def one_block(block_args):
        q_blk, seg_blk, pos_blk = block_args
        scores = jnp.einsum('qkgd,tkd->kgqt', q_blk.astype(jnp.float32), key_f32) * q_scale
        pos_gap = pos_blk[:, None] - positions[None, :]
        allowed = (seg_blk[:, None] == seg_ids[None, :]) & (pos_gap >= 0) & (pos_gap < window)
        scores = jnp.where(allowed[None, None], scores, -1e30)
        row_max = jnp.max(scores, axis=-1, keepdims=True)
        exp_scores = jnp.exp(scores - row_max)
        probs_bf = (exp_scores / jnp.sum(exp_scores, axis=-1, keepdims=True)).astype(jnp.bfloat16)
        blk_out = jnp.einsum('kgqt,tkd->qkgd', probs_bf.astype(jnp.float32), value_f32)
        return blk_out.astype(jnp.bfloat16)

    attn_out = lax.map(one_block, (q_blocks, seg_blocks, pos_blocks))
    return attn_out.reshape(TOKENS, Q_HEADS * HEAD_DIM)


def run_layer(hidden, seg_ids, positions, layer_w, norm_row, qk_row, rope_base, pos_factor, window):
    w_query, w_key, w_value, w_out, w_gate, w_up, w_down = layer_w
    resid_f32 = hidden.astype(jnp.float32)
    normed = gemma_norm(resid_f32, norm_row[0]).astype(jnp.bfloat16)
    query_bf = jnp.dot(normed, w_query, preferred_element_type=jnp.float32).astype(jnp.bfloat16)
    keys_bf = jnp.dot(normed, w_key, preferred_element_type=jnp.float32).astype(jnp.bfloat16)
    values_bf = jnp.dot(normed, w_value, preferred_element_type=jnp.float32).astype(jnp.bfloat16)
    cos_tab, sin_tab = rope_tables(positions, rope_base, pos_factor)
    query_heads = apply_rope(gemma_norm(query_bf.astype(jnp.float32).reshape(TOKENS, Q_HEADS, HEAD_DIM), qk_row[0]), cos_tab, sin_tab).astype(jnp.bfloat16)
    key_heads = apply_rope(gemma_norm(keys_bf.astype(jnp.float32).reshape(TOKENS, KV_HEADS, HEAD_DIM), qk_row[1]), cos_tab, sin_tab).astype(jnp.bfloat16)
    value_heads = values_bf.reshape(TOKENS, KV_HEADS, HEAD_DIM)
    attn_out = attend(query_heads, key_heads, value_heads, seg_ids, positions, window)
    attn_sum = jnp.dot(attn_out, w_out, preferred_element_type=jnp.float32).astype(jnp.bfloat16)
    hidden_mid = (resid_f32 + gemma_norm(attn_sum.astype(jnp.float32), norm_row[1])).astype(jnp.bfloat16)
    mid_f32 = hidden_mid.astype(jnp.float32)
    normed_ffn = gemma_norm(mid_f32, norm_row[2]).astype(jnp.bfloat16)
    gate_bf = jnp.dot(normed_ffn, w_gate, preferred_element_type=jnp.float32).astype(jnp.bfloat16)
    up_bf = jnp.dot(normed_ffn, w_up, preferred_element_type=jnp.float32).astype(jnp.bfloat16)
    ffn_in = (jax.nn.gelu(gate_bf.astype(jnp.float32), approximate=True) * up_bf.astype(jnp.float32)).astype(jnp.bfloat16)
    ffn_sum = jnp.dot(ffn_in, w_down, preferred_element_type=jnp.float32).astype(jnp.bfloat16)
    hidden_new = (mid_f32 + gemma_norm(ffn_sum.astype(jnp.float32), norm_row[3])).astype(jnp.bfloat16)
    return hidden_new, key_heads, value_heads


def reference(hidden_in, seg_ids, positions, w_query, w_key, w_value, w_out, w_gate, w_up, w_down, norm_scales, qk_scales):
    settings = ((GLOBAL_BASE, GLOBAL_FACTOR, TOKENS), (LOCAL_BASE, 1.0, WINDOW))
    hidden = hidden_in
    key_list = []
    value_list = []
    for layer_idx in range(2):
        rope_base, pos_factor, window = settings[layer_idx]
        layer_w = (w_query[layer_idx], w_key[layer_idx], w_value[layer_idx], w_out[layer_idx], w_gate[layer_idx], w_up[layer_idx], w_down[layer_idx])
        hidden, key_heads, value_heads = run_layer(hidden, seg_ids, positions, layer_w, norm_scales[layer_idx], qk_scales[layer_idx], rope_base, pos_factor, window)
        key_list.append(key_heads)
        value_list.append(value_heads)
    return hidden, jnp.stack(key_list), jnp.stack(value_list)
```

```python
import functools

import jax
import jax.numpy as jnp
from jax import lax
from jax.experimental import pallas as pl
from jax.experimental.pallas import tpu as pltpu
from jax.sharding import PartitionSpec as P

NORM_EPS = 1e-6
WINDOW = 1024
GLOBAL_BASE = 1000000.0
GLOBAL_FACTOR = 8.0
LOCAL_BASE = 10000.0
LOG2E = 1.4426950408889634
NEG = -1e30
F32 = jnp.float32
BF16 = jnp.bfloat16


def mm(a, b):
    return jnp.dot(a, b, preferred_element_type=F32)


def qkv_kernel(xa_ref, xb_ref, sc_ref, wqa, wqb, wka, wkb, wva, wvb, cos_ref, sin_ref, qks_ref,
               q_ref, k_ref, v_ref):
    half = xa_ref.shape[1]
    xa = xa_ref[...].astype(F32)
    xb = xb_ref[...].astype(F32)
    ss = jnp.sum(xa * xa, axis=-1, keepdims=True) + jnp.sum(xb * xb, axis=-1, keepdims=True)
    r = lax.rsqrt(ss / (2 * half) + NORM_EPS)
    ha = (xa * r * (1.0 + sc_ref[:, :half])).astype(BF16)
    hb = (xb * r * (1.0 + sc_ref[:, half:])).astype(BF16)
    cos = cos_ref[...]
    sin = sin_ref[...]
    hd = qks_ref.shape[1]
    h2 = hd // 2

    def finish(t, scale_row):
        t = t.astype(BF16).astype(F32)
        t = t * lax.rsqrt(jnp.mean(t * t, axis=-1, keepdims=True) + NORM_EPS) * (1.0 + scale_row)
        a, b = t[:, :h2], t[:, h2:]
        return jnp.concatenate([a * cos - b * sin, b * cos + a * sin], axis=-1).astype(BF16)

    q = mm(ha, wqa[...]) + mm(hb, wqb[...])
    for n in range(q.shape[1] // hd):
        q_ref[:, n * hd:(n + 1) * hd] = finish(q[:, n * hd:(n + 1) * hd], qks_ref[0:1, :])
    k_ref[...] = finish(mm(ha, wka[...]) + mm(hb, wkb[...]), qks_ref[1:2, :])
    v_ref[...] = (mm(ha, wva[...]) + mm(hb, wvb[...])).astype(BF16)


def qkv_call(layer, xa, xb, b_col, scales, ws, cos, sin, qks, blk=512):
    n = xa.shape[0]
    half = ws[0].shape[1]
    wq, wqp, wk, wkp, wv, wvp = ws
    hd = qks.shape[-1]

    def wspec(w):
        return pl.BlockSpec((None,) + w.shape[1:], lambda i: (layer, 0, 0))

    flops = 2 * n * 2 * half * (wq.shape[2] + 2 * wk.shape[2])
    return pl.pallas_call(
        qkv_kernel,
        name="qkv%d" % layer,
        grid=(n // blk,),
        in_specs=[pl.BlockSpec((blk, half), lambda i: (i, 0)),
                  pl.BlockSpec((blk, half), lambda i: (i, b_col)),
                  pl.BlockSpec((None, 1, 2 * half), lambda i: (layer * 4, 0, 0))] +
                 [wspec(w) for w in ws] +
                 [pl.BlockSpec((blk, hd // 2), lambda i: (i, 0)),
                  pl.BlockSpec((blk, hd // 2), lambda i: (i, 0)),
                  pl.BlockSpec((None, 2, hd), lambda i: (layer, 0, 0))],
        out_specs=[pl.BlockSpec((blk, wq.shape[2]), lambda i: (i, 0)),
                   pl.BlockSpec((blk, hd), lambda i: (i, 0)),
                   pl.BlockSpec((blk, hd), lambda i: (i, 0))],
        out_shape=[jax.ShapeDtypeStruct((n, wq.shape[2]), BF16),
                   jax.ShapeDtypeStruct((n, hd), BF16),
                   jax.ShapeDtypeStruct((n, hd), BF16)],
        compiler_params=pltpu.CompilerParams(dimension_semantics=("arbitrary",), vmem_limit_bytes=60 * 2**20),
        cost_estimate=pl.CostEstimate(flops=flops, bytes_accessed=n * 2 * half * 2 + n * 4 * hd * 2, transcendentals=0),
    )(xa, xb, scales, *ws, cos, sin, qks)


def attn_kernel(bq, bk, lo_min, lo_max, q_ref, k_ref, v_ref, lo_ref, o_ref, m_ref, l_ref, acc_ref):
    i = pl.program_id(0)
    q_start = i * bq
    m_ref[...] = jnp.full_like(m_ref, NEG)
    l_ref[...] = jnp.zeros_like(l_ref)
    acc_ref[...] = jnp.zeros_like(acc_ref)
    c = LOG2E * (q_ref.shape[1] ** -0.5)

    def step(jb, masked):
        k_blk = k_ref[pl.ds(pl.multiple_of(jb * bk, bk), bk), :]
        v_blk = v_ref[pl.ds(pl.multiple_of(jb * bk, bk), bk), :]
        s = lax.dot_general(q_ref[...], k_blk, (((1,), (1,)), ((), ())), preferred_element_type=F32) * c
        if masked:
            row = q_start + lax.broadcasted_iota(jnp.int32, (bq, bk), 0)
            col = jb * bk + lax.broadcasted_iota(jnp.int32, (bq, bk), 1)
            s = jnp.where((col <= row) & (col >= lo_ref[...]), s, NEG)
        m_prev = m_ref[...]
        m_new = jnp.maximum(m_prev, jnp.max(s, axis=1, keepdims=True))
        p = jnp.exp2(s - m_new[:, :1])
        alpha = jnp.exp2(m_prev - m_new)
        l_ref[...] = alpha * l_ref[...] + jnp.sum(p, axis=1, keepdims=True)
        acc_ref[...] = acc_ref[...] * alpha[:, :1] + mm(p.astype(BF16), v_blk)
        m_ref[...] = m_new

    start = lo_min[i] // bk
    end = (q_start + bq - 1) // bk + 1
    a = jnp.minimum(jnp.maximum(start, (lo_max[i] + bk - 1) // bk), end)
    b = jnp.minimum(jnp.maximum(a, (q_start + 1) // bk), end)

    @pl.loop(start, a)
    def _(jb):
        step(jb, True)

    @pl.loop(a, b)
    def _(jb):
        step(jb, False)

    @pl.loop(b, end)
    def _(jb):
        step(jb, True)

    o_ref[...] = (acc_ref[...] / l_ref[:, :1]).astype(BF16)


def attn_call(layer, q, k, v, lo, bq=512, bk=512):
    n, hd = q.shape
    lo_b = lo.reshape(n // bq, bq)
    full = pl.BlockSpec((n, hd), lambda i, *_: (0, 0))
    return pl.pallas_call(
        functools.partial(attn_kernel, bq, bk),
        name="attn%d" % layer,
        grid_spec=pltpu.PrefetchScalarGridSpec(
            num_scalar_prefetch=2,
            grid=(n // bq,),
            in_specs=[pl.BlockSpec((bq, hd), lambda i, *_: (i, 0)), full, full,
                      pl.BlockSpec((bq, 1), lambda i, *_: (i, 0))],
            out_specs=pl.BlockSpec((bq, hd), lambda i, *_: (i, 0)),
            scratch_shapes=[pltpu.VMEM((bq, 128), F32), pltpu.VMEM((bq, 128), F32), pltpu.VMEM((bq, hd), F32)]),
        out_shape=jax.ShapeDtypeStruct((n, hd), BF16),
        compiler_params=pltpu.CompilerParams(dimension_semantics=("arbitrary",), vmem_limit_bytes=48 * 2**20),
        cost_estimate=pl.CostEstimate(flops=4 * n * n * hd // 4, bytes_accessed=4 * n * hd * 2, transcendentals=n * n // 4),
    )(lo_b[:, 0], lo_b[:, -1], q, k, v, lo[:, None])


def out_kernel(o_ref, wa_ref, wb_ref, xa_ref, xb_ref, s1_ref, s2_ref, x1_ref, h_ref):
    half = xa_ref.shape[1]
    width = 2 * half
    o = jnp.concatenate([o_ref[s] for s in range(o_ref.shape[0])], axis=-1)
    rows = o.shape[1]
    aa = mm(o, wa_ref[...].reshape(rows, half)).astype(BF16).astype(F32)
    ab = mm(o, wb_ref[...].reshape(rows, half)).astype(BF16).astype(F32)

    def rs(a, b):
        ss = jnp.sum(a * a, axis=-1, keepdims=True) + jnp.sum(b * b, axis=-1, keepdims=True)
        return lax.rsqrt(ss / width + NORM_EPS)

    r = rs(aa, ab)
    xa = (xa_ref[...].astype(F32) + aa * r * (1.0 + s1_ref[:, :half])).astype(BF16)
    xb = (xb_ref[...].astype(F32) + ab * r * (1.0 + s1_ref[:, half:])).astype(BF16)
    x1_ref[:, :half] = xa
    x1_ref[:, half:] = xb
    xa = xa.astype(F32)
    xb = xb.astype(F32)
    r = rs(xa, xb)
    h_ref[:, :half] = (xa * r * (1.0 + s2_ref[:, :half])).astype(BF16)
    h_ref[:, half:] = (xb * r * (1.0 + s2_ref[:, half:])).astype(BF16)


def out_call(layer, o, wa, wb, xa, xb, b_col, scales, blk=256):
    g, n, hd = o.shape
    half = wa.shape[-1]
    wspec = pl.BlockSpec((wa.shape[0], None) + wa.shape[2:], lambda i: (0, layer, 0, 0))
    sds = jax.ShapeDtypeStruct((n, 2 * half), BF16)
    return pl.pallas_call(
        out_kernel,
        name="out%d" % layer,
        grid=(n // blk,),
        in_specs=[pl.BlockSpec((g, blk, hd), lambda i: (0, i, 0)), wspec, wspec,
                  pl.BlockSpec((blk, half), lambda i: (i, 0)),
                  pl.BlockSpec((blk, half), lambda i: (i, b_col)),
                  pl.BlockSpec((None, 1, 2 * half), lambda i: (layer * 4 + 1, 0, 0)),
                  pl.BlockSpec((None, 1, 2 * half), lambda i: (layer * 4 + 2, 0, 0))],
        out_specs=[pl.BlockSpec((blk, 2 * half), lambda i: (i, 0))] * 2,
        out_shape=[sds, sds],
        compiler_params=pltpu.CompilerParams(dimension_semantics=("arbitrary",), vmem_limit_bytes=60 * 2**20),
        cost_estimate=pl.CostEstimate(flops=2 * n * g * hd * 2 * half, bytes_accessed=g * hd * 2 * half * 2, transcendentals=0),
    )(o, wa, wb, xa, xb, scales, scales)


def ffn_kernel(has_init, *refs):
    if has_init:
        h_ref, ga, gb, ua, ub, da, db, init_ref, out_ref = refs
    else:
        h_ref, ga, gb, ua, ub, da, db, out_ref = refs
    half = ga.shape[0]
    j = pl.program_id(0)

    @pl.when(j == 0)
    def _():
        if has_init:
            out_ref[...] = init_ref[...]
        else:
            out_ref[...] = jnp.zeros_like(out_ref)

    ha = h_ref[:, :half]
    hb = h_ref[:, half:]
    g = (mm(ha, ga[...]) + mm(hb, gb[...])).astype(BF16).astype(F32)
    u = (mm(ha, ua[...]) + mm(hb, ub[...])).astype(BF16).astype(F32)
    m = (jax.nn.gelu(g, approximate=True) * u).astype(BF16)
    out_ref[:, :half] += mm(m, da[...])
    out_ref[:, half:] += mm(m, db[...])


def ffn_call(layer, tag, h, ws, init=None, fblk=256):
    n, width = h.shape
    ga = ws[0]
    ff = ga.shape[-1]

    def wspec(w, down):
        shape = (fblk, width // 2) if down else (width // 2, fblk)
        if w.ndim == 3:
            return pl.BlockSpec((None,) + shape, (lambda j: (layer, j, 0)) if down else (lambda j: (layer, 0, j)))
        return pl.BlockSpec(shape, (lambda j: (j, 0)) if down else (lambda j: (0, j)))

    full = pl.BlockSpec((n, width), lambda j: (0, 0))
    args = [h, *ws] + ([init] if init is not None else [])
    specs = [full] + [wspec(w, i >= 4) for i, w in enumerate(ws)] + ([full] if init is not None else [])
    return pl.pallas_call(
        functools.partial(ffn_kernel, init is not None),
        name="ffn%d%s" % (layer, tag),
        grid=(ff // fblk,),
        in_specs=specs,
        out_specs=full,
        out_shape=jax.ShapeDtypeStruct((n, width), F32),
        compiler_params=pltpu.CompilerParams(dimension_semantics=("arbitrary",), vmem_limit_bytes=60 * 2**20),
        cost_estimate=pl.CostEstimate(flops=6 * n * width * ff, bytes_accessed=3 * width * ff * 2 + n * width * 6, transcendentals=n * ff),
    )(*args)


def rope_tables(positions, head_dim, rope_base, pos_factor):
    exponents = jnp.arange(0, head_dim, 2).astype(F32) / head_dim
    inv_freq = rope_base ** (-exponents)
    angles = (positions.astype(F32) / pos_factor)[:, None] * inv_freq[None, :]
    return jnp.cos(angles), jnp.sin(angles)


def solution(mesh):
    n_heads = mesh.shape['heads']
    n_model = mesh.shape['model']
    n_dev = n_heads * n_model
    col_spec = P(None, 'model', 'heads')
    row_spec = P(None, 'heads', 'model')
    cache_spec = P(None, None, 'heads', None)
    core_pairs = [(i, n_model - 1 - i) for i in range(n_model)]

    def swap_core(v):
        return lax.ppermute(v, 'model', core_pairs)

    def swap_chip(v, bit):
        return lax.ppermute(v, 'heads', [(i, i ^ bit) for i in range(n_heads)])

    def body(hidden_in, seg_ids, positions, w_query, w_key, w_value, w_out, w_gate, w_up, w_down, norm_scales, qk_scales):
        n_tok, half = hidden_in.shape
        hd = qk_scales.shape[-1]
        own_n = n_tok // n_dev
        hi = lax.axis_index('heads')
        mi = lax.axis_index('model')

        def pick(v, m):
            return lax.dynamic_index_in_dim(v, m, axis=1, keepdims=False)

        def by_core(own, other, axis):
            first = mi == 0
            return jnp.stack([jnp.where(first, own, other), jnp.where(first, other, own)], axis=axis)

        hid = hidden_in.reshape(n_heads, n_model, own_n, half)
        xa = pick(hid, mi).reshape(-1, half)
        xb = swap_core(pick(hid, 1 - mi).reshape(-1, half))
        wq_p, wk_p, wv_p = swap_core(w_query), swap_core(w_key), swap_core(w_value)
        qkv_w = (w_query, wq_p, w_key, wk_p, w_value, wv_p)
        scales = jnp.concatenate([norm_scales, swap_core(norm_scales)], axis=-1).reshape(-1, 1, 2 * half)

        wo_a = lax.all_gather(w_out, 'heads', axis=0)
        wo_b = swap_core(wo_a)
        own_w = (w_gate, w_up, w_down)
        own_wp = tuple(swap_core(w) for w in own_w)
        nbr_bits = (1, 2)
        nbr_w = [tuple(swap_chip(w[l], nbr_bits[l]) for w in own_w) for l in range(2)]
        nbr_wp = [tuple(swap_core(w) for w in nbr_w[l]) for l in range(2)]

        def interleave(a, b):
            return [t for pair in zip(a, b) for t in pair]

        my_pos = pick(positions.reshape(n_heads, n_model, own_n), mi).reshape(-1)
        tok = jnp.arange(n_tok, dtype=jnp.int32)
        settings = ((GLOBAL_BASE, GLOBAL_FACTOR, n_tok), (LOCAL_BASE, 1.0, WINDOW))
        keys, values = [], []
        x_own = None
        b_col = 0
        for l in range(2):
            base, factor, window = settings[l]
            cos, sin = rope_tables(my_pos, hd, base, factor)
            q, k, v = qkv_call(l, xa, xb, b_col, scales, qkv_w, cos, sin, qk_scales)
            q_other = jnp.where(mi == 0, q[:, hd:], q[:, :hd])
            q_mine = jnp.where(mi == 0, q[:, :hd], q[:, hd:])
            q_r, k_r, v_r = swap_core(q_other), swap_core(k), swap_core(v)

            def whole(own, other):
                return by_core(own.reshape(n_heads, own_n, hd), other.reshape(n_heads, own_n, hd), 1).reshape(n_tok, hd)

            q_all, k_all, v_all = whole(q_mine, q_r), whole(k, k_r), whole(v, v_r)
            keys.append(k_all)
            values.append(v_all)
            lo = tok - jnp.minimum(positions, window - 1)
            o = attn_call(l, q_all, k_all, v_all, lo)
            o = lax.all_to_all(o.reshape(n_dev, own_n, hd), ('heads', 'model'), split_axis=0, concat_axis=0, tiled=True)
            if l == 0:
                ra = lax.dynamic_slice_in_dim(xa, hi * own_n, own_n, 0)
                rb = lax.dynamic_slice_in_dim(xb, hi * own_n, own_n, 0)
                x1, h2 = out_call(l, o, wo_a, wo_b, ra, rb, 0, scales)
            else:
                x1, h2 = out_call(l, o, wo_a, wo_b, x_own, x_own, 1, scales)
            act_bit = 3 - nbr_bits[l]
            h2_r = swap_chip(h2, act_bit)
            w_own = interleave(own_w, own_wp)
            w_nbr = interleave(nbr_w[l], nbr_wp[l])
            p_own = ffn_call(l, "a", h2, w_own)
            p_rem = ffn_call(l, "b", h2_r, w_own)
            p_rem = ffn_call(l, "c", h2_r, w_nbr, p_rem)
            p_got = swap_chip(p_rem, act_bit)
            p_own = ffn_call(l, "d", h2, w_nbr, p_own)
            f = (p_own + p_got).astype(BF16).astype(F32)
            r = lax.rsqrt(jnp.mean(f * f, axis=-1, keepdims=True) + NORM_EPS)
            x_own = (x1.astype(F32) + f * r * (1.0 + scales[l * 4 + 3])).astype(BF16)
            if l == 0:
                xg = lax.all_gather(x_own, 'heads', axis=0, tiled=True)
                xa, xb, b_col = xg, xg, 1
        other = swap_core(x_own[:, half:])
        both = by_core(x_own[:, :half], other, 0).reshape(n_model * own_n, half)
        hidden = lax.all_gather(both, 'heads', axis=0, tiled=True)
        return hidden, jnp.stack(keys)[:, :, None, :], jnp.stack(values)[:, :, None, :]

    return jax.shard_map(body, mesh=mesh,
                         in_specs=(P(None, 'model'), P(), P(), col_spec, col_spec, col_spec, row_spec, col_spec, col_spec, row_spec, P(None, None, 'model'), P()),
                         out_specs=(P(None, 'model'), cache_spec, cache_spec),
                         check_vma=False)
```
